512 devices in a mesh: stack: 2 (over y), date: 8 (over x), line: 32 (over z, core).
Axes of the slice: x: 8, y: 2, z: 16, core: 2. Of those that a mesh axis runs over, the one named last changes fastest.
The devices are a block of a 8x8x16 slice.
Arguments:
- slc: float32 [8, 2, 512, 10240], P('date', None, 'stack', 'line'), parts along dimension 2, may hold values from -6 to 6
- band_start: int32 [8], replicated, may hold values from 0 to 5120, as said below
- band_stop: int32 [8], replicated, may hold values from 5120 to 10240, as said below
Outputs:
- interferogram: float32 [8, 2, 512, 2048], P('date', None, 'stack', 'line'), parts along dimension 2
The draws below stay inside these ranges and needn't reach their ends.
There are 2 independent parts, one for each index of `stack`. The reference program is written for one: setup_inputs(seed, part) draws one part's arguments, and reference() takes and returns one part's arrays. A program takes and returns all parts, laid end to end along the dimension named above; an argument that names none is the same for every part. Nothing has to cross between parts.
Inputs may be any that keep to these rules, and one draw needn't show every extreme that they name: For every pair, band_stop - band_start lies between 5120 and 7680; at least one pair keeps exactly 7680 bins, and some pair keeps exactly 5120 bins ending at 10240. `band_stop`: see band_start.
All inputs are finite; a program needn't handle non-finite values.
Results may differ from the reference program's by a relative error of at most 0.0001.
Values sent between devices are 32-bit elements; how exact they have to be, the bound alone decides.
A program may use at most 64 MiB of HBM per device.

```python
import jax
import jax.numpy as jnp

COLS = 256
LOOKS = 5
LINES = 10240
DATES = 8


def band_pair(key):
    key_width = jax.random.fold_in(key, 11)
    key_chosen = jax.random.fold_in(key, 23)
    key_offset = jax.random.fold_in(key, 37)
    narrowest = LINES // 2
    widest = 3 * LINES // 4
    order = jax.random.permutation(key_chosen, jnp.arange(DATES, dtype=jnp.int32))
    pair_ids = jnp.arange(DATES, dtype=jnp.int32)
    widths = jax.random.randint(key_width, (DATES,), narrowest, widest + 1)
    widths = jnp.where(pair_ids == order[0], widest, widths)
    widths = jnp.where((pair_ids == order[1]) | (pair_ids == order[2]), narrowest, widths)
    starts = jax.random.randint(key_offset, (DATES,), 0, LINES - widths + 1)
    starts = jnp.where(pair_ids == order[1], LINES - narrowest, starts)
    starts = jnp.where(pair_ids == order[2], 0, starts)
    return (starts.astype(jnp.int32), (starts + widths).astype(jnp.int32))


def draw_band_start(key, part):
    return band_pair(key)[0]


def draw_band_stop(key, part):
    return band_pair(key)[1]


def steps_of(own_key, shape, split, least, largest):
    factor_of, own = 1.0, jax.random.fold_in(own_key, 6)
    for dim, parts in split:
        steps = jnp.exp(jax.random.uniform(jax.random.fold_in(own, dim), (parts,), jnp.float32, least / len(split), largest / len(split)))
        factor_of = factor_of * jnp.repeat(steps, shape[dim] // parts).reshape([-1 if axis == dim else 1 for axis in range(len(shape))])
    return factor_of


def normal_values(key, dims, width, bound, pieces=(), kind=jnp.bfloat16):
    gain = steps_of(key, dims, pieces, -0.22, 0.18) if pieces else 1.0
    drawn = jax.random.normal(key, dims, jnp.float32) * width * gain
    return jnp.minimum(jnp.maximum(drawn, -bound), bound).astype(kind)


def setup_inputs(seed: int = 0, part: int = 0) -> dict:
    key_of = jax.random.split(jax.random.key(seed), 4)
    part_splits = jax.random.split(jax.random.fold_in(key_of[3], part), 4)
    return {
        "slc": normal_values(part_splits[0], (DATES, 2, COLS, LINES), 1.0, 6.0, ((0, 8), (3, 32)), jnp.float32),
        "band_start": draw_band_start(jax.random.fold_in(key_of[3], 71), part),
        "band_stop": draw_band_stop(jax.random.fold_in(key_of[3], 71), part),
    }


def reference(slc, band_start, band_stop):
    images = slc[:, 0] + 1j * slc[:, 1]
    spectra = jnp.fft.fft(images, axis=-1)
    partner = jnp.roll(spectra, -1, axis=0)
    bins_all = jnp.arange(LINES, dtype=jnp.int32)
    keep_mask = (bins_all[None, :] >= band_start[:, None]) & (bins_all[None, :] < band_stop[:, None])
    keep_mask = keep_mask[:, None, :]
    ref_signal = jnp.fft.ifft(jnp.where(keep_mask, spectra, 0), axis=-1)
    sec_signal = jnp.fft.ifft(jnp.where(keep_mask, partner, 0), axis=-1)
    product = ref_signal * jnp.conj(sec_signal)
    looked = product.reshape(DATES, COLS, LINES // LOOKS, LOOKS).mean(axis=-1)
    return jnp.stack([jnp.real(looked), jnp.imag(looked)], axis=1).astype(jnp.float32)
```

```python
import functools
import math

import jax
import jax.numpy as jnp
import numpy as np
from jax import lax
from jax.experimental import pallas as pl
from jax.experimental.pallas import tpu as pltpu
from jax.sharding import PartitionSpec as P

LOOKS = 5
CORES = 2
GROUP = 4
LANES = 128
MESH = pl.DeviceIdType.MESH


def split_table(table):
    high = table.astype(jnp.bfloat16)
    low = (table - high.astype(np.float32)).astype(jnp.bfloat16)
    return np.stack([high, low])


@functools.lru_cache(maxsize=None)
def tables(outer, inner):
    whole = outer * inner
    bins = 2 * LANES
    tail = inner - bins
    eye = np.eye(GROUP)
    turn = 2 * np.pi / outer * (np.outer(np.arange(outer), np.arange(outer)) % outer)
    cos, sin = np.cos(turn), np.sin(turn)
    blocks = np.array([[cos, sin], [-sin, cos]])
    first = np.einsum("pqkd,x->pkdqx", blocks, np.ones(GROUP)).reshape(2 * outer, -1)
    last = np.einsum("qdk,cx->dcqxk", np.array([cos, sin]), eye).reshape(outer * GROUP, -1)
    line, bin_ = np.arange(inner), np.arange(bins)
    turn = 2 * np.pi / inner * (np.outer(line, bin_) % inner)
    cos, sin = np.cos(turn), np.sin(turn)
    from_re = np.concatenate([cos, -sin], 1)
    from_im = np.concatenate([sin, cos], 1)
    ahead = np.concatenate([from_re[:bins], from_im[:bins], from_re[bins:], from_im[bins:]])
    looks = inner // LOOKS
    order = (np.arange(looks)[None] * LOOKS + np.arange(LOOKS)[:, None]).reshape(-1)
    cos_o, sin_o = cos[order].T, sin[order].T
    to_re = np.concatenate([cos_o, -sin_o], 0).reshape(2 * bins, LOOKS, 1, looks)
    to_im = np.concatenate([sin_o, cos_o], 0).reshape(2 * bins, LOOKS, 1, looks)
    back = np.concatenate([to_re, to_im], 2).reshape(2 * bins, 2 * inner)
    k1 = np.arange(outer)
    lanes = np.concatenate([line, line[bins:]])
    turn = 2 * np.pi / whole * np.outer(k1, lanes)
    ahead_turn = np.stack([np.cos(turn), -np.sin(turn)])
    turn = 2 * np.pi / whole * np.outer(k1, order)
    cos, sin = (f(turn).reshape(-1, LOOKS, 1, looks) for f in (np.cos, np.sin))
    back_turn = np.stack(
        [
            np.concatenate([cos, cos], 2).reshape(-1, 2 * inner),
            np.concatenate([-sin, sin], 2).reshape(-1, 2 * inner),
        ]
    )
    assert 2 * tail == LANES and 2 * looks == LANES
    as_f32 = lambda a: a.astype(np.float32)
    return (
        split_table(as_f32(first)),
        split_table(as_f32(ahead)),
        split_table(as_f32(back)),
        split_table(as_f32(last)),
        as_f32(ahead_turn),
        as_f32(back_turn),
    )


def parts_of(values):
    high = values.astype(jnp.bfloat16)
    return high, (values - high.astype(jnp.float32)).astype(jnp.bfloat16)


def dot(a, b):
    return jnp.dot(a, b, preferred_element_type=jnp.float32)


def left(table, values):
    high, low = parts_of(values)
    return dot(table[0], high) + dot(table[0], low) + dot(table[1], high)


def right(values, table):
    high, low = parts_of(values)
    return dot(high, table[0]) + dot(low, table[0]) + dot(high, table[1])


def half_turned(values, roll):
    pieces = [
        roll(values[:, i : i + LANES]) for i in range(0, values.shape[1], LANES)
    ]
    return jnp.concatenate(pieces, 1)


def lane_index(shape):
    return lax.broadcasted_iota(jnp.int32, shape, 1)


def low_half(shape):
    return lane_index(shape) % LANES < LANES // 2


def start_turn(ahead_turn, start, outer, inner):
    lanes = lane_index((1, 3 * LANES))
    line = jnp.where(lanes < inner, lanes, lanes - (LANES // 2))
    steps = (line * (start // outer)).astype(jnp.float32)
    steps = steps - inner * jnp.floor((steps + 0.5) * (1.0 / inner))
    angle = steps * (2.0 * math.pi / inner)
    cos, sin = jnp.cos(angle), -jnp.sin(angle)
    real, imag = ahead_turn[0], ahead_turn[1]
    return for_columns(real * cos - imag * sin), for_columns(real * sin + imag * cos)


def first_table(first, outer):
    column = lane_index((2 * outer, first.shape[2])) % GROUP
    pieces = []
    for piece in (first[0], first[1]):
        wide = piece.astype(jnp.float32)
        own = [jnp.where(column == c, wide, 0.0) for c in range(GROUP)]
        rows = [v[:outer] for v in own] + [v[outer:] for v in own]
        pieces.append(jnp.concatenate(rows, 0).astype(jnp.bfloat16))
    return pieces


def for_columns(table):
    return jnp.concatenate([table] * GROUP, 0)


def lines_of(first, tiles, turn, second, roll):
    block = jnp.concatenate(tiles, 1)
    mixed = left(first, block)
    rows = mixed.shape[0] // 2
    real, imag = mixed[:rows], mixed[rows:]
    turned_real = real * turn[0] - imag * turn[1]
    turned_imag = real * turn[1] + imag * turn[0]
    main = 2 * LANES
    tail_real, tail_imag = turned_real[:, main:], turned_imag[:, main:]
    low = low_half(tail_real.shape)
    if second:
        tail = jnp.where(low, roll(tail_real), tail_imag)
    else:
        tail = jnp.where(low, tail_real, roll(tail_imag))
    return jnp.concatenate([turned_real[:, :main], turned_imag[:, :main], tail], 1)


def keep_mask(start, stop, outer, rows):
    shape = (rows, 2 * LANES)
    k1 = lax.broadcasted_iota(jnp.int32, shape, 0) % outer
    k = k1 + outer * (lane_index(shape) + start // outer)
    return (k >= start) & (k < stop)


def back_lines(spectrum, mask, back, back_turn, roll):
    bins = mask.shape[1]
    kept = jnp.concatenate(
        [jnp.where(mask, spectrum[:, :bins], 0.0), jnp.where(mask, spectrum[:, bins:], 0.0)], 1
    )
    lines = right(kept, back)
    return lines * for_columns(back_turn[0]) + half_turned(lines, roll) * for_columns(back_turn[1])


def signal_of(lines, last, roll):
    turned = half_turned(lines, roll)
    turned = jnp.where(low_half(turned.shape), -turned, turned)
    return left(last, jnp.concatenate([lines, turned], 0))


def looked(ref, sec, scale, roll):
    same = cross = None
    for i in range(LOOKS):
        a, b = (v[:, i * LANES : (i + 1) * LANES] for v in (ref, sec))
        one, two = a * b, a * roll(b)
        same = one if same is None else same + one
        cross = two if cross is None else cross + two
    low = low_half(same.shape)
    return jnp.where(low, same + roll(same), cross - roll(cross)) * scale


def tpu_roll(values):
    return pltpu.roll(values, LANES // 2, 1)


def ring_order(size):
    order = [size // 2]
    for step in range(size // 2 - 1, 0, -1):
        order += [step, size - step]
    return order


def kernel(
    chips, inner,
    x_ref, start_ref, stop_ref,
    first, ahead, back, last, ahead_turn, back_turn,
    out_ref,
    image, packed, own, far_a, far_b, spec, sends, gather, mixing,
    load_sem, send_sem, own_sem, pass_sem, far_sem, back_send, back_recv,
):
    devices = chips * CORES
    me = lax.axis_index("line")
    chip = me // CORES
    partner = chip * CORES + (CORES - 1 - me % CORES)
    date = lax.axis_index("date")
    dates = lax.axis_size("date")
    before = lax.rem(date + dates - 1, dates)
    after = lax.rem(date + 1, dates)
    load = pltpu.make_async_copy(x_ref.at[0], image, load_sem)
    load.start()

    barrier = pltpu.get_barrier_semaphore()

    def greet(i, _):
        pl.semaphore_signal(
            barrier, 1, device_id={"line": lax.rem(me + i, devices)}, device_id_type=MESH
        )
        return 0

    lax.fori_loop(1, devices, greet, 0)
    for row in (before, after):
        pl.semaphore_signal(barrier, 1, device_id={"date": row}, device_id_type=MESH)

    for i, piece in enumerate(first_table(first, devices)):
        mixing[i] = piece
    load.wait()

    def pack(t, _):
        rows = pl.ds(pl.multiple_of(t * 2 * GROUP, 2 * GROUP), 2 * GROUP)
        for k in range(2):
            lanes = slice(k * LANES, (k + 1) * LANES)
            real, imag = image[0, rows, lanes], image[1, rows, lanes]
            packed[t, k] = jnp.concatenate([real[:GROUP], imag[:GROUP]], 0)
            packed[t, 3 + k] = jnp.concatenate([real[GROUP:], imag[GROUP:]], 0)
        lanes = slice(2 * LANES, inner)
        real, imag = image[0, rows, lanes], image[1, rows, lanes]
        packed[t, 2] = jnp.concatenate(
            [
                jnp.concatenate([real[:GROUP], imag[:GROUP]], 0),
                jnp.concatenate([real[GROUP:], imag[GROUP:]], 0),
            ],
            1,
        )
        return 0

    lax.fori_loop(0, devices, pack, 0)
    pl.semaphore_wait(barrier, devices + 1)

    tiles = (pl.ds(0, 3), pl.ds(3, 2))
    order = ring_order(chips)

    def send(t, c):
        pltpu.make_async_remote_copy(
            packed.at[t, tiles[c]], own.at[me, tiles[c]], send_sem.at[c], own_sem.at[c, chip],
            device_id={"line": t}, device_id_type=MESH,
        ).start()

    for c in range(2):
        for o in order:
            t = lax.rem(chip + o, chips)
            for core in range(CORES):
                send(t * CORES + core, c)
        send(partner, c)
    own[me] = packed[me]

    passed = (pl.ds(0, 3), pl.ds(2, 3))
    fars = (far_a, far_b)
    rows_to = (before, after)

    def pass_on(s, c):
        pltpu.make_async_remote_copy(
            own.at[s, passed[c]], fars[c].at[s], pass_sem.at[c], far_sem.at[c],
            device_id={"date": rows_to[c]}, device_id_type=MESH,
        ).start()

    def take(c):
        one = own.at[pl.ds(0, 1), tiles[c]]
        pltpu.make_async_copy(one, one, own_sem.at[c, chip]).wait()
        for s in (me, partner):
            pass_on(s, c)
        for o in order:
            s = lax.rem(chip + chips - o, chips)
            both = own.at[pl.ds(0, CORES), tiles[c]]
            pltpu.make_async_copy(both, both, own_sem.at[c, s]).wait()
            for core in range(CORES):
                pass_on(s * CORES + core, c)

    rows = devices * GROUP
    scale = 1.0 / (LOOKS * float(devices * inner) ** 2)

    def tile(ref, k):
        return ref[:, k].reshape(2 * rows, LANES)

    def work(c):
        pair = (date, before)[c]
        start, stop = start_ref[pair], stop_ref[pair]
        turn = start_turn(ahead_turn, start, devices, inner)
        mine = [tile(own, k) for k in ((0, 1, 2), (3, 4, 2))[c]]
        theirs = [tile(fars[c], k) for k in ((0, 1, 2), (1, 2, 0))[c]]
        both = [mine, theirs] if c == 0 else [theirs, mine]
        lines = jnp.concatenate([lines_of(mixing, v, turn, c == 1, tpu_roll) for v in both], 0)
        spec[...] = right(lines, ahead)
        mask = keep_mask(start, stop, devices, rows)
        signals = []
        for i in range(2):
            part = spec[i * rows : (i + 1) * rows]
            signals.append(
                signal_of(back_lines(part, mask, back, back_turn, tpu_roll), last, tpu_roll)
            )
        result = looked(*signals, scale, tpu_roll)
        sends[c] = result.reshape(devices, GROUP, LANES)

    def give(c):
        row = (date, before)[c]
        skip = (1, 0)[c]

        def one(i, _):
            t = lax.rem(i + (me if skip else 0), devices)
            pltpu.make_async_remote_copy(
                sends.at[c, t], gather.at[c, me], back_send.at[c], back_recv.at[c],
                device_id={"line": t, "date": row}, device_id_type=MESH,
            ).start()
            return 0

        lax.fori_loop(skip, devices, one, 0)
        if skip:
            gather[c, me] = sends[c, me]

    def far_done(c):
        pltpu.make_async_copy(fars[c], fars[c], far_sem.at[c]).wait()

    take(0)
    far_done(0)
    work(0)
    give(0)
    take(1)
    far_done(1)
    work(1)
    give(1)

    for c in range(2):
        sent = own.at[pl.ds(0, devices - 1), tiles[c]]
        pltpu.make_async_copy(sent, sent, send_sem.at[c]).wait()
        pltpu.make_async_copy(fars[c], fars[c], pass_sem.at[c]).wait()
        whole = gather.at[c, pl.ds(0, devices - (1, 0)[c])]
        for sem in (back_send, back_recv):
            pltpu.make_async_copy(whole, whole, sem.at[c]).wait()

    half = LANES // 2
    joined = jnp.concatenate([gather[0], gather[1]], 1).reshape(2 * rows, LANES)
    out_ref[0, 0] = joined[:, :half]
    out_ref[0, 1] = joined[:, half:]


def shards(slc, band_start, band_stop):
    devices = lax.axis_size("line")
    chips = devices // CORES
    _, parts, columns, inner = slc.shape
    rows = devices * GROUP
    half = LANES // 2
    assert columns == devices * 2 * GROUP and inner == 2 * LANES + half
    constants = tables(devices, inner)
    hbm = pl.BlockSpec(memory_space=pltpu.HBM)
    vmem = pl.BlockSpec(memory_space=pltpu.VMEM)
    smem = pl.BlockSpec(memory_space=pltpu.SMEM)
    dma = pltpu.SemaphoreType.DMA
    f32 = jnp.float32
    return pl.pallas_call(
        functools.partial(kernel, chips, inner),
        out_shape=jax.ShapeDtypeStruct((1, parts, columns, inner // LOOKS), f32),
        in_specs=[hbm, smem, smem] + [vmem] * len(constants),
        out_specs=vmem,
        scratch_shapes=[
            pltpu.VMEM((parts, columns, inner), f32),
            pltpu.VMEM((devices, 5, 2 * GROUP, LANES), f32),
            pltpu.VMEM((devices, 5, 2 * GROUP, LANES), f32),
            pltpu.VMEM((devices, 3, 2 * GROUP, LANES), f32),
            pltpu.VMEM((devices, 3, 2 * GROUP, LANES), f32),
            pltpu.VMEM((2 * rows, 4 * LANES), f32),
            pltpu.VMEM((2, devices, GROUP, LANES), f32),
            pltpu.VMEM((2, devices, GROUP, LANES), f32),
            pltpu.VMEM((2, 2 * rows, 2 * rows), jnp.bfloat16),
            dma,
            dma((2,)),
            dma((2, chips)),
            dma((2,)),
            dma((2,)),
            dma((2,)),
            dma((2,)),
        ],
        compiler_params=pltpu.CompilerParams(collective_id=0, has_side_effects=True),
    )(slc, band_start, band_stop, *(jnp.asarray(c) for c in constants))


def solution(mesh):
    return jax.shard_map(
        shards,
        mesh=mesh,
        in_specs=(P("date", None, "stack", "line"), P(), P()),
        out_specs=P("date", None, "stack", "line"),
        check_vma=False,
    )
```

```python
import functools
import math

import jax
import jax.numpy as jnp
import numpy as np
from jax import lax
from jax.experimental import pallas as pl
from jax.experimental.pallas import tpu as pltpu
from jax.sharding import PartitionSpec as P

LOOKS = 5
CORES = 2
GROUP = 4
EARLY = 5
LANES = 128
MESH = pl.DeviceIdType.MESH


def split_table(table):
    high = table.astype(jnp.bfloat16)
    low = (table - high.astype(np.float32)).astype(jnp.bfloat16)
    return np.stack([high, low])


@functools.lru_cache(maxsize=None)
def tables(outer, inner):
    whole = outer * inner
    bins = 2 * LANES
    tail = inner - bins
    eye = np.eye(GROUP)
    turn = 2 * np.pi / outer * (np.outer(np.arange(outer), np.arange(outer)) % outer)
    cos, sin = np.cos(turn), np.sin(turn)
    blocks = np.array([[cos, sin], [-sin, cos]])
    first = np.einsum("pqkd,x->pkdqx", blocks, np.ones(GROUP)).reshape(2 * outer, -1)
    last = np.einsum("qdk,cx->dcqxk", np.array([cos, sin]), eye).reshape(outer * GROUP, -1)
    line, bin_ = np.arange(inner), np.arange(bins)
    turn = 2 * np.pi / inner * (np.outer(line, bin_) % inner)
    cos, sin = np.cos(turn), np.sin(turn)
    from_re = np.concatenate([cos, -sin], 1)
    from_im = np.concatenate([sin, cos], 1)
    ahead = np.concatenate([from_re[:bins], from_im[:bins], from_re[bins:], from_im[bins:]])
    looks = inner // LOOKS
    order = (np.arange(looks)[None] * LOOKS + np.arange(LOOKS)[:, None]).reshape(-1)
    cos_o, sin_o = cos[order].T, sin[order].T
    to_re = np.concatenate([cos_o, -sin_o], 0).reshape(2 * bins, LOOKS, 1, looks)
    to_im = np.concatenate([sin_o, cos_o], 0).reshape(2 * bins, LOOKS, 1, looks)
    back = np.concatenate([to_re, to_im], 2).reshape(2 * bins, 2 * inner)
    k1 = np.arange(outer)
    lanes = np.concatenate([line, line[bins:]])
    turn = 2 * np.pi / whole * np.outer(k1, lanes)
    ahead_turn = np.stack([np.cos(turn), -np.sin(turn)])
    turn = 2 * np.pi / whole * np.outer(k1, order)
    cos, sin = (f(turn).reshape(-1, LOOKS, 1, looks) for f in (np.cos, np.sin))
    back_turn = np.stack(
        [
            np.concatenate([cos, cos], 2).reshape(-1, 2 * inner),
            np.concatenate([-sin, sin], 2).reshape(-1, 2 * inner),
        ]
    )
    assert 2 * tail == LANES and 2 * looks == LANES
    as_f32 = lambda a: a.astype(np.float32)
    return (
        split_table(as_f32(first)),
        split_table(as_f32(ahead)),
        split_table(as_f32(back)),
        split_table(as_f32(last)),
        as_f32(ahead_turn),
        as_f32(back_turn),
    )


def parts_of(values):
    high = values.astype(jnp.bfloat16)
    return high, (values - high.astype(jnp.float32)).astype(jnp.bfloat16)


def dot(a, b):
    return jnp.dot(a, b, preferred_element_type=jnp.float32)


def left(table, values):
    high, low = parts_of(values)
    return dot(table[0], high) + dot(table[0], low) + dot(table[1], high)


def right(values, table):
    high, low = parts_of(values)
    return dot(high, table[0]) + dot(low, table[0]) + dot(high, table[1])


def half_turned(values, roll):
    pieces = [
        roll(values[:, i : i + LANES]) for i in range(0, values.shape[1], LANES)
    ]
    return jnp.concatenate(pieces, 1)


def lane_index(shape):
    return lax.broadcasted_iota(jnp.int32, shape, 1)


def low_half(shape):
    return lane_index(shape) % LANES < LANES // 2


def start_turn(ahead_turn, start, outer, inner):
    lanes = lane_index((1, 3 * LANES))
    line = jnp.where(lanes < inner, lanes, lanes - (LANES // 2))
    steps = (line * (start // outer)).astype(jnp.float32)
    steps = steps - inner * jnp.floor((steps + 0.5) * (1.0 / inner))
    angle = steps * (2.0 * math.pi / inner)
    cos, sin = jnp.cos(angle), -jnp.sin(angle)
    real, imag = ahead_turn[0], ahead_turn[1]
    return for_columns(real * cos - imag * sin), for_columns(real * sin + imag * cos)


def first_table(first, outer):
    column = lane_index((2 * outer, first.shape[2])) % GROUP
    pieces = []
    for piece in (first[0], first[1]):
        wide = piece.astype(jnp.float32)
        own = [jnp.where(column == c, wide, 0.0) for c in range(GROUP)]
        rows = [v[:outer] for v in own] + [v[outer:] for v in own]
        pieces.append(jnp.concatenate(rows, 0).astype(jnp.bfloat16))
    return pieces


def for_columns(table):
    return jnp.concatenate([table] * GROUP, 0)


def lines_of(first, tiles, turn, second, roll):
    block = jnp.concatenate(tiles, 1)
    mixed = left(first, block)
    rows = mixed.shape[0] // 2
    real, imag = mixed[:rows], mixed[rows:]
    turned_real = real * turn[0] - imag * turn[1]
    turned_imag = real * turn[1] + imag * turn[0]
    main = 2 * LANES
    tail_real, tail_imag = turned_real[:, main:], turned_imag[:, main:]
    low = low_half(tail_real.shape)
    tail = jnp.where(
        second,
        jnp.where(low, roll(tail_real), tail_imag),
        jnp.where(low, tail_real, roll(tail_imag)),
    )
    return jnp.concatenate([turned_real[:, :main], turned_imag[:, :main], tail], 1)


def keep_mask(start, stop, outer, rows):
    shape = (rows, 2 * LANES)
    k1 = lax.broadcasted_iota(jnp.int32, shape, 0) % outer
    k = k1 + outer * (lane_index(shape) + start // outer)
    return (k >= start) & (k < stop)


def back_lines(spectrum, mask, back, back_turn, roll):
    bins = mask.shape[1]
    kept = jnp.concatenate(
        [jnp.where(mask, spectrum[:, :bins], 0.0), jnp.where(mask, spectrum[:, bins:], 0.0)], 1
    )
    lines = right(kept, back)
    return lines * for_columns(back_turn[0]) + half_turned(lines, roll) * for_columns(back_turn[1])


def signal_of(lines, last, roll):
    turned = half_turned(lines, roll)
    turned = jnp.where(low_half(turned.shape), -turned, turned)
    return left(last, jnp.concatenate([lines, turned], 0))


def looked(ref, sec, scale, roll):
    same = cross = None
    for i in range(LOOKS):
        a, b = (v[:, i * LANES : (i + 1) * LANES] for v in (ref, sec))
        one, two = a * b, a * roll(b)
        same = one if same is None else same + one
        cross = two if cross is None else cross + two
    low = low_half(same.shape)
    return jnp.where(low, same + roll(same), cross - roll(cross)) * scale


def tpu_roll(values):
    return pltpu.roll(values, LANES // 2, 1)


def ring_order(size):
    order = [size // 2]
    for step in range(size // 2 - 1, 0, -1):
        order += [step, size - step]
    return order


def sublanes_turned(values):
    return pltpu.roll(values, GROUP, 1)


def pack(image, packed, inner):
    columns = image.shape[2]
    for h in range(columns // LANES):
        lanes = slice(h * LANES, (h + 1) * LANES)
        count = LANES // (2 * GROUP)
        to = slice(h * count, (h + 1) * count)
        shape = (count, 2 * GROUP, LANES)
        upper = lax.broadcasted_iota(jnp.int32, shape, 1) < GROUP
        for k in range(2):
            lines = slice(k * LANES, (k + 1) * LANES)
            real, imag = (image[i, lines, lanes].T.reshape(shape) for i in range(2))
            packed[to, k] = jnp.where(upper, real, sublanes_turned(imag))
            packed[to, 3 + k] = jnp.where(upper, sublanes_turned(real), imag)
        tail = jnp.concatenate([image[i, 2 * LANES : inner, lanes] for i in range(2)], 0)
        tail = tail.T
        other = pltpu.roll(tail, LANES // 2, 1).reshape(shape)
        tail = tail.reshape(shape)
        low = lax.broadcasted_iota(jnp.int32, shape, 2) < LANES // 2
        packed[to, 2] = jnp.where(upper == low, tail, sublanes_turned(other))


def kernel(
    chips, early, inner,
    x_ref, start_hbm, stop_hbm,
    first_hbm, ahead_hbm, back_hbm, last_hbm, ahead_turn_hbm, back_turn_hbm,
    out_ref,
    image, packed, own, spec, sends, gather, mixing,
    start_ref, stop_ref, first, ahead, back, last, ahead_turn, back_turn,
    load_sem, table_sem, ready, known, prior, send_sem, own_sem, pass_sem, far_sem, back_send, back_recv,
):
    devices = chips * CORES
    me = lax.axis_index("line")
    chip = me // CORES
    partner = chip * CORES + (CORES - 1 - me % CORES)
    date = lax.axis_index("date")
    dates = lax.axis_size("date")
    before = lax.rem(date + dates - 1, dates)
    after = lax.rem(date + 1, dates)
    load = pltpu.make_async_copy(x_ref.at[0], image, load_sem)
    load.start()

    hubs = early - 1
    hub = (me >= 1) & (me < early)
    barrier = pltpu.get_barrier_semaphore()

    def signal(sem, line):
        pl.semaphore_signal(sem, 1, device_id={"line": line}, device_id_type=MESH)

    def loop(low, high, body):
        def step(i, _):
            body(i)
            return 0

        lax.fori_loop(low, high, step, 0)

    def others(low, high, body):
        loop(low, high, lambda i: pl.when(i != me)(lambda: body(i)))

    @pl.when(hub)
    def _():
        others(0, devices, lambda t: signal(barrier, t))

    for row in (before, after):
        pl.semaphore_signal(barrier, 1, device_id={"date": row}, device_id_type=MESH)

    moves = [
        pltpu.make_async_copy(source, to, table_sem.at[i])
        for i, (source, to) in enumerate(
            (
                (first_hbm, first), (start_hbm, start_ref), (stop_hbm, stop_ref),
                (ahead_turn_hbm, ahead_turn), (ahead_hbm, ahead), (back_hbm, back),
                (back_turn_hbm, back_turn), (last_hbm, last),
            )
        )
    ]

    @pl.when(jnp.logical_not(hub))
    def _():
        pl.semaphore_wait(barrier, hubs + 2)
        loop(1, early, lambda t: signal(ready.at[chip], t))

    load.wait()
    for move in moves:
        move.start()
    pack(image, packed, inner)

    @pl.when(hub)
    def _():
        pl.semaphore_wait(barrier, hubs + 1)

    tiles = (pl.ds(0, 3), pl.ds(3, 2))
    order = ring_order(chips)

    def send(t, c):
        pltpu.make_async_remote_copy(
            packed.at[t, tiles[c]], own.at[me, tiles[c]], send_sem.at[c], own_sem.at[c, chip],
            device_id={"line": t}, device_id_type=MESH,
        ).start()

    def ring(body):
        for o in order:
            t = lax.rem(chip + o, chips) * CORES
            for core in range(CORES):
                body(t + core)
        body(partner)

    for c in range(2):
        ring(lambda t: pl.when((t >= 1) & (t < early))(lambda: send(t, c)))

    def send_both(t):
        for c in range(2):
            send(t, c)

    def send_chip(k):
        for core in range(CORES):
            send_both(k * CORES + core)

    first_chip = early // CORES

    @pl.when(hub)
    def _():
        teller = me == 1

        def meet(k):
            pl.semaphore_wait(ready.at[k], CORES)

            @pl.when(teller)
            def _():
                for core in range(CORES):
                    signal(prior, k * CORES + core)
                loop(early, k * CORES, lambda t: signal(known.at[k], t))
                pl.when(k == chips - 1)(lambda: signal(known.at[k], 0))

            send_chip(k)

        loop(first_chip, chips - 1, meet)
        pl.semaphore_wait(ready.at[0], 1)

        @pl.when(teller)
        def _():
            signal(prior, 0)
            loop(early, devices - CORES, lambda t: signal(known.at[0], t))

        send_both(0)
        meet(chips - 1)

    @pl.when(jnp.logical_not(hub))
    def _():
        zero = me == 0
        end = chip == chips - 1
        pl.semaphore_wait(prior, 1)
        pl.when(jnp.logical_not(zero))(lambda: send_both(partner))
        pl.when(end)(lambda: send_both(0))
        loop(first_chip, jnp.where(zero, chips - 1, chip), send_chip)

        def meet(k):
            pl.semaphore_wait(known.at[k], 1)
            send_chip(k)

        loop(jnp.where(zero, chips, chip + 1), chips - 1, meet)

        @pl.when(jnp.logical_not(zero | end))
        def _():
            pl.semaphore_wait(known.at[0], 1)
            send_both(0)

        pl.when(jnp.logical_not(end))(lambda: meet(chips - 1))

    own[me, 0:5] = packed[me]
    for move in moves:
        move.wait()
    for i, piece in enumerate(first_table(first, devices)):
        mixing[i] = piece

    passed = (pl.ds(0, 3), pl.ds(2, 3))
    passed_to = (pl.ds(5, 3), pl.ds(8, 3))
    rows_to = (before, after)

    def pass_on(s, c):
        pltpu.make_async_remote_copy(
            own.at[s, passed[c]], own.at[s, passed_to[c]], pass_sem.at[c], far_sem.at[c],
            device_id={"date": rows_to[c]}, device_id_type=MESH,
        ).start()

    def take(s, count):
        for c in range(2):
            new = own.at[pl.ds(0, count), tiles[c]]
            pltpu.make_async_copy(new, new, own_sem.at[c, s]).wait()
            for core in range(CORES):
                pass_on(s * CORES + core, c)

    rows = devices * GROUP
    scale = 1.0 / (LOOKS * float(devices * inner) ** 2)

    def tile(k):
        return own[:, k].reshape(2 * rows, LANES)

    def image_signal(c, far):
        pair = jnp.where(c == 0, date, before)
        start, stop = start_ref[pair], stop_ref[pair]
        turn = start_turn(ahead_turn, start, devices, inner)
        main = 3 * c + far * (5 + c)
        tail = 2 + far * (5 + c)
        block = [tile(main), tile(main + 1), tile(tail)]
        lines = lines_of(mixing, block, turn, c == 1, tpu_roll)
        mask = keep_mask(start, stop, devices, rows)
        kept = back_lines(right(lines, ahead), mask, back, back_turn, tpu_roll)
        return signal_of(kept, last, tpu_roll)

    def give(c):
        row = jnp.where(c == 0, date, before)

        def one(t):
            pltpu.make_async_remote_copy(
                sends.at[c, t], gather.at[c, me], back_send.at[c], back_recv.at[c],
                device_id={"line": t, "date": row}, device_id_type=MESH,
            ).start()

        loop(0, devices, lambda t: pl.when((c == 1) | (t != me))(lambda: one(t)))

        @pl.when(c == 0)
        def _():
            gather[c, me] = sends[c, me]

    take(chip, 1)
    for o in order[::-1]:
        take(lax.rem(chip + chips - o, chips), CORES)

    def image_of(i):
        c, far = lax.rem(i, 2), i // 2

        @pl.when(far == 1)
        def _():
            new = own.at[:, pl.ds(5, 3)]
            pltpu.make_async_copy(new, new, far_sem.at[c]).wait()

        spec[i] = image_signal(c, far)

        @pl.when(far == 1)
        def _():
            ref, sec = spec[i - 2 + 2 * c], spec[i - 2 * c]
            sends[c] = looked(ref, sec, scale, tpu_roll).reshape(devices, GROUP, LANES)
            give(c)

    loop(0, 4, image_of)

    for c in range(2):
        whole = gather.at[c, pl.ds(0, devices - (1, 0)[c])]
        pltpu.make_async_copy(whole, whole, back_recv.at[c]).wait()

    half = LANES // 2
    joined = jnp.concatenate([gather[0], gather[1]], 1).reshape(2 * rows, LANES)
    for h in range(2 * rows // LANES):
        lanes = slice(h * LANES, (h + 1) * LANES)
        both = joined[lanes].T
        out_ref[0, 0, :, lanes] = both[:half]
        out_ref[0, 1, :, lanes] = both[half:]

    for c in range(2):
        sent = own.at[pl.ds(0, devices - 1), tiles[c]]
        pltpu.make_async_copy(sent, sent, send_sem.at[c]).wait()
        new = own.at[:, pl.ds(5, 3)]
        pltpu.make_async_copy(new, new, pass_sem.at[c]).wait()
        whole = gather.at[c, pl.ds(0, devices - (1, 0)[c])]
        pltpu.make_async_copy(whole, whole, back_send.at[c]).wait()


def shards(slc, band_start, band_stop):
    devices = lax.axis_size("line")
    chips = devices // CORES
    _, parts, columns, inner = slc.shape
    rows = devices * GROUP
    half = LANES // 2
    assert columns == devices * 2 * GROUP and inner == 2 * LANES + half
    constants = [jnp.asarray(c) for c in tables(devices, inner)]
    hbm = pl.BlockSpec(memory_space=pltpu.HBM)
    dma = pltpu.SemaphoreType.DMA
    count = pltpu.SemaphoreType.REGULAR
    f32 = jnp.float32
    result = pl.pallas_call(
        functools.partial(kernel, chips, EARLY * devices // 8, inner),
        out_shape=jax.ShapeDtypeStruct((1, parts, inner // LOOKS, columns), f32),
        in_specs=[hbm] * (3 + len(constants)),
        out_specs=pl.BlockSpec(memory_space=pltpu.VMEM),
        scratch_shapes=[
            pltpu.VMEM((parts, inner, columns), f32),
            pltpu.VMEM((devices, 5, 2 * GROUP, LANES), f32),
            pltpu.VMEM((devices, 11, 2 * GROUP, LANES), f32),
            pltpu.VMEM((4, rows, 2 * inner), f32),
            pltpu.VMEM((2, devices, GROUP, LANES), f32),
            pltpu.VMEM((2, devices, GROUP, LANES), f32),
            pltpu.VMEM((2, 2 * rows, 2 * rows), jnp.bfloat16),
            pltpu.SMEM(band_start.shape, jnp.int32),
            pltpu.SMEM(band_stop.shape, jnp.int32),
            *(pltpu.VMEM(c.shape, c.dtype) for c in constants),
            dma,
            dma((8,)),
            count((chips,)),
            count((chips,)),
            count,
            dma((2,)),
            dma((2, chips)),
            dma((2,)),
            dma((2,)),
            dma((2,)),
            dma((2,)),
        ],
        compiler_params=pltpu.CompilerParams(collective_id=0, has_side_effects=True),
    )(jnp.swapaxes(slc, 2, 3), band_start, band_stop, *constants)
    return jnp.swapaxes(result, 2, 3)


def solution(mesh):
    return jax.shard_map(
        shards,
        mesh=mesh,
        in_specs=(P("date", None, "stack", "line"), P(), P()),
        out_specs=P("date", None, "stack", "line"),
        check_vma=False,
    )
```

```python
import functools
import math

import jax
import jax.numpy as jnp
import numpy as np
from jax import lax
from jax.experimental import pallas as pl
from jax.experimental.pallas import tpu as pltpu
from jax.sharding import PartitionSpec as P

LOOKS = 5
CORES = 2
GROUP = 4
EARLY = 5
LANES = 128
MESH = pl.DeviceIdType.MESH


def split_table(table):
    high = table.astype(jnp.bfloat16)
    low = (table - high.astype(np.float32)).astype(jnp.bfloat16)
    return np.stack([high, low])


@functools.lru_cache(maxsize=None)
def tables(outer, inner):
    whole = outer * inner
    bins = 2 * LANES
    tail = inner - bins
    eye = np.eye(GROUP)
    turn = 2 * np.pi / outer * (np.outer(np.arange(outer), np.arange(outer)) % outer)
    cos, sin = np.cos(turn), np.sin(turn)
    blocks = np.array([[cos, sin], [-sin, cos]])
    first = np.einsum("pqkd,x->pkdqx", blocks, np.ones(GROUP)).reshape(2 * outer, -1)
    last = np.einsum("qdk,cx->dcqxk", np.array([cos, sin]), eye).reshape(outer * GROUP, -1)
    line, bin_ = np.arange(inner), np.arange(bins)
    turn = 2 * np.pi / inner * (np.outer(line, bin_) % inner)
    cos, sin = np.cos(turn), np.sin(turn)
    from_re = np.concatenate([cos, -sin], 1)
    from_im = np.concatenate([sin, cos], 1)
    ahead = np.concatenate([from_re[:bins], from_im[:bins], from_re[bins:], from_im[bins:]])
    looks = inner // LOOKS
    order = (np.arange(looks)[None] * LOOKS + np.arange(LOOKS)[:, None]).reshape(-1)
    cos_o, sin_o = cos[order].T, sin[order].T
    to_re = np.concatenate([cos_o, -sin_o], 0).reshape(2 * bins, LOOKS, 1, looks)
    to_im = np.concatenate([sin_o, cos_o], 0).reshape(2 * bins, LOOKS, 1, looks)
    back = np.concatenate([to_re, to_im], 2).reshape(2 * bins, 2 * inner)
    k1 = np.arange(outer)
    lanes = np.concatenate([line, line[bins:]])
    turn = 2 * np.pi / whole * np.outer(k1, lanes)
    ahead_turn = np.stack([np.cos(turn), -np.sin(turn)])
    turn = 2 * np.pi / whole * np.outer(k1, order)
    cos, sin = (f(turn).reshape(-1, LOOKS, 1, looks) for f in (np.cos, np.sin))
    back_turn = np.stack(
        [
            np.concatenate([cos, cos], 2).reshape(-1, 2 * inner),
            np.concatenate([-sin, sin], 2).reshape(-1, 2 * inner),
        ]
    )
    assert 2 * tail == LANES and 2 * looks == LANES
    as_f32 = lambda a: a.astype(np.float32)
    return (
        split_table(as_f32(first)),
        split_table(as_f32(ahead)),
        split_table(as_f32(back)),
        split_table(as_f32(last)),
        as_f32(ahead_turn),
        as_f32(back_turn),
    )


def parts_of(values):
    high = values.astype(jnp.bfloat16)
    return high, (values - high.astype(jnp.float32)).astype(jnp.bfloat16)


def dot(a, b):
    return jnp.dot(a, b, preferred_element_type=jnp.float32)


def left(table, values):
    high, low = parts_of(values)
    return dot(table[0], high) + dot(table[0], low) + dot(table[1], high)


def right(values, table):
    high, low = parts_of(values)
    return dot(high, table[0]) + dot(low, table[0]) + dot(high, table[1])


def half_turned(values, roll):
    pieces = [
        roll(values[:, i : i + LANES]) for i in range(0, values.shape[1], LANES)
    ]
    return jnp.concatenate(pieces, 1)


def lane_index(shape):
    return lax.broadcasted_iota(jnp.int32, shape, 1)


def low_half(shape):
    return lane_index(shape) % LANES < LANES // 2


def start_turn(ahead_turn, start, outer, inner):
    lanes = lane_index((1, 3 * LANES))
    line = jnp.where(lanes < inner, lanes, lanes - (LANES // 2))
    steps = (line * (start // outer)).astype(jnp.float32)
    steps = steps - inner * jnp.floor((steps + 0.5) * (1.0 / inner))
    angle = steps * (2.0 * math.pi / inner)
    cos, sin = jnp.cos(angle), -jnp.sin(angle)
    real, imag = ahead_turn[0], ahead_turn[1]
    return for_columns(real * cos - imag * sin), for_columns(real * sin + imag * cos)


def first_table(first, outer):
    column = lane_index((2 * outer, first.shape[2])) % GROUP
    pieces = []
    for piece in (first[0], first[1]):
        wide = piece.astype(jnp.float32)
        own = [jnp.where(column == c, wide, 0.0) for c in range(GROUP)]
        rows = [v[:outer] for v in own] + [v[outer:] for v in own]
        pieces.append(jnp.concatenate(rows, 0).astype(jnp.bfloat16))
    return pieces


def for_columns(table):
    return jnp.concatenate([table] * GROUP, 0)


def lines_of(first, tiles, turn, second, roll):
    block = jnp.concatenate(tiles, 1)
    mixed = left(first, block)
    rows = mixed.shape[0] // 2
    real, imag = mixed[:rows], mixed[rows:]
    turned_real = real * turn[0] - imag * turn[1]
    turned_imag = real * turn[1] + imag * turn[0]
    main = 2 * LANES
    tail_real, tail_imag = turned_real[:, main:], turned_imag[:, main:]
    low = low_half(tail_real.shape)
    tail = jnp.where(
        second,
        jnp.where(low, roll(tail_real), tail_imag),
        jnp.where(low, tail_real, roll(tail_imag)),
    )
    return jnp.concatenate([turned_real[:, :main], turned_imag[:, :main], tail], 1)


def keep_mask(start, stop, outer, rows):
    shape = (rows, 2 * LANES)
    k1 = lax.broadcasted_iota(jnp.int32, shape, 0) % outer
    k = k1 + outer * (lane_index(shape) + start // outer)
    return (k >= start) & (k < stop)


def back_lines(spectrum, mask, back, back_turn, roll):
    bins = mask.shape[1]
    kept = jnp.concatenate(
        [jnp.where(mask, spectrum[:, :bins], 0.0), jnp.where(mask, spectrum[:, bins:], 0.0)], 1
    )
    lines = right(kept, back)
    return lines * for_columns(back_turn[0]) + half_turned(lines, roll) * for_columns(back_turn[1])


def signal_of(lines, last, roll):
    turned = half_turned(lines, roll)
    turned = jnp.where(low_half(turned.shape), -turned, turned)
    return left(last, jnp.concatenate([lines, turned], 0))


def looked(ref, sec, scale, roll):
    same = cross = None
    for i in range(LOOKS):
        a, b = (v[:, i * LANES : (i + 1) * LANES] for v in (ref, sec))
        one, two = a * b, a * roll(b)
        same = one if same is None else same + one
        cross = two if cross is None else cross + two
    low = low_half(same.shape)
    return jnp.where(low, same + roll(same), cross - roll(cross)) * scale


def tpu_roll(values):
    return pltpu.roll(values, LANES // 2, 1)


def ring_order(size):
    order = [size // 2]
    for step in range(size // 2 - 1, 0, -1):
        order += [step, size - step]
    return order


def sublanes_turned(values):
    return pltpu.roll(values, GROUP, 1)


def pack(image, packed, inner):
    columns = image.shape[2]
    for h in range(columns // LANES):
        lanes = slice(h * LANES, (h + 1) * LANES)
        count = LANES // (2 * GROUP)
        to = slice(h * count, (h + 1) * count)
        shape = (count, 2 * GROUP, LANES)
        upper = lax.broadcasted_iota(jnp.int32, shape, 1) < GROUP
        for k in range(2):
            lines = slice(k * LANES, (k + 1) * LANES)
            real, imag = (image[i, lines, lanes].T.reshape(shape) for i in range(2))
            packed[to, k] = jnp.where(upper, real, sublanes_turned(imag))
            packed[to, 3 + k] = jnp.where(upper, sublanes_turned(real), imag)
        tail = jnp.concatenate([image[i, 2 * LANES : inner, lanes] for i in range(2)], 0)
        tail = tail.T
        other = pltpu.roll(tail, LANES // 2, 1).reshape(shape)
        tail = tail.reshape(shape)
        low = lax.broadcasted_iota(jnp.int32, shape, 2) < LANES // 2
        packed[to, 2] = jnp.where(upper == low, tail, sublanes_turned(other))


def kernel(
    chips, early, inner,
    x_ref, start_hbm, stop_hbm,
    first_hbm, ahead_hbm, back_hbm, last_hbm, ahead_turn_hbm, back_turn_hbm,
    out_ref,
    image, packed, own, spec, sends, gather, mixing,
    start_ref, stop_ref, first, ahead, back, last, ahead_turn, back_turn,
    load_sem, table_sem, ready, known, prior, send_sem, own_sem, pass_sem, far_sem, back_send, back_recv,
):
    devices = chips * CORES
    me = lax.axis_index("line")
    chip = me // CORES
    partner = chip * CORES + (CORES - 1 - me % CORES)
    date = lax.axis_index("date")
    dates = lax.axis_size("date")
    before = lax.rem(date + dates - 1, dates)
    after = lax.rem(date + 1, dates)
    load = pltpu.make_async_copy(x_ref.at[0], image, load_sem)
    load.start()

    hubs = early - 1
    hub = (me >= 1) & (me < early)
    barrier = pltpu.get_barrier_semaphore()

    def signal(sem, line):
        pl.semaphore_signal(sem, 1, device_id={"line": line}, device_id_type=MESH)

    def loop(low, high, body):
        def step(i, _):
            body(i)
            return 0

        lax.fori_loop(low, high, step, 0)

    def others(low, high, body):
        loop(low, high, lambda i: pl.when(i != me)(lambda: body(i)))

    @pl.when(hub)
    def _():
        others(0, devices, lambda t: signal(barrier, t))

    for row in (before, after):
        pl.semaphore_signal(barrier, 1, device_id={"date": row}, device_id_type=MESH)

    moves = [
        pltpu.make_async_copy(source, to, table_sem.at[i])
        for i, (source, to) in enumerate(
            (
                (first_hbm, first), (start_hbm, start_ref), (stop_hbm, stop_ref),
                (ahead_turn_hbm, ahead_turn), (ahead_hbm, ahead), (back_hbm, back),
                (back_turn_hbm, back_turn), (last_hbm, last),
            )
        )
    ]

    @pl.when(jnp.logical_not(hub))
    def _():
        pl.semaphore_wait(barrier, hubs + 2)
        loop(1, early, lambda t: signal(ready.at[chip], t))

    load.wait()
    for move in moves:
        move.start()
    pack(image, packed, inner)

    @pl.when(hub)
    def _():
        pl.semaphore_wait(barrier, hubs + 1)

    tiles = (pl.ds(0, 3), pl.ds(3, 2))
    order = ring_order(chips)

    def send(t, c):
        pltpu.make_async_remote_copy(
            packed.at[t, tiles[c]], own.at[me, tiles[c]], send_sem.at[c], own_sem.at[c, chip],
            device_id={"line": t}, device_id_type=MESH,
        ).start()

    def ring(body):
        for o in order:
            t = lax.rem(chip + o, chips) * CORES
            for core in range(CORES):
                body(t + core)
        body(partner)

    for c in range(2):
        ring(lambda t: pl.when((t >= 1) & (t < early))(lambda: send(t, c)))

    def send_both(t):
        for c in range(2):
            send(t, c)

    def send_chip(k):
        for core in range(CORES):
            send_both(k * CORES + core)

    first_chip = early // CORES

    @pl.when(hub)
    def _():
        teller = me == 1

        def meet(k):
            pl.semaphore_wait(ready.at[k], CORES)

            @pl.when(teller)
            def _():
                for core in range(CORES):
                    signal(prior, k * CORES + core)
                loop(early, k * CORES, lambda t: signal(known.at[k], t))
                pl.when(k == chips - 1)(lambda: signal(known.at[k], 0))

            send_chip(k)

        loop(first_chip, chips - 1, meet)
        pl.semaphore_wait(ready.at[0], 1)

        @pl.when(teller)
        def _():
            signal(prior, 0)
            loop(early, devices - CORES, lambda t: signal(known.at[0], t))

        send_both(0)
        meet(chips - 1)

    @pl.when(jnp.logical_not(hub))
    def _():
        zero = me == 0
        end = chip == chips - 1
        pl.semaphore_wait(prior, 1)
        pl.when(jnp.logical_not(zero))(lambda: send_both(partner))
        pl.when(end)(lambda: send_both(0))
        loop(first_chip, jnp.where(zero, chips - 1, chip), send_chip)

        def meet(k):
            pl.semaphore_wait(known.at[k], 1)
            send_chip(k)

        loop(jnp.where(zero, chips, chip + 1), chips - 1, meet)

        @pl.when(jnp.logical_not(zero | end))
        def _():
            pl.semaphore_wait(known.at[0], 1)
            send_both(0)

        pl.when(jnp.logical_not(end))(lambda: meet(chips - 1))

    own[me, 0:5] = packed[me]
    for move in moves:
        move.wait()
    for i, piece in enumerate(first_table(first, devices)):
        mixing[i] = piece

    passed = (pl.ds(0, 3), pl.ds(2, 3))
    passed_to = (pl.ds(5, 3), pl.ds(8, 3))
    rows_to = (before, after)

    def pass_on(s, c):
        pltpu.make_async_remote_copy(
            own.at[s, passed[c]], own.at[s, passed_to[c]], pass_sem.at[c], far_sem.at[c],
            device_id={"date": rows_to[c]}, device_id_type=MESH,
        ).start()

    def take(s, count):
        for c in range(2):
            new = own.at[pl.ds(0, count), tiles[c]]
            pltpu.make_async_copy(new, new, own_sem.at[c, s]).wait()
            for core in range(CORES):
                pass_on(s * CORES + core, c)

    rows = devices * GROUP
    scale = 1.0 / (LOOKS * float(devices * inner) ** 2)

    def tile(k):
        return own[:, k].reshape(2 * rows, LANES)

    def image_signal(c, far):
        pair = jnp.where(c == 0, date, before)
        start, stop = start_ref[pair], stop_ref[pair]
        turn = start_turn(ahead_turn, start, devices, inner)
        main = 3 * c + far * (5 + c)
        tail = 2 + far * (5 + c)
        block = [tile(main), tile(main + 1), tile(tail)]
        lines = lines_of(mixing, block, turn, c == 1, tpu_roll)
        mask = keep_mask(start, stop, devices, rows)
        kept = back_lines(right(lines, ahead), mask, back, back_turn, tpu_roll)
        return signal_of(kept, last, tpu_roll)

    def give(c, low, high):
        row = jnp.where(c == 0, date, before)

        def one(t):
            pltpu.make_async_remote_copy(
                sends.at[c, t], gather.at[c, me], back_send.at[c], back_recv.at[c],
                device_id={"line": t, "date": row}, device_id_type=MESH,
            ).start()

        loop(low, high, lambda t: pl.when((c == 1) | (t != me))(lambda: one(t)))

    take(chip, 1)
    loop(1, chips - 1, lambda s: pl.when(s != chip)(lambda: take(s, CORES)))
    pl.when(chip != 0)(lambda: take(0, CORES))
    pl.when(chip != chips - 1)(lambda: take(chips - 1, CORES))

    def image_of(i):
        c, far = lax.rem(i, 2), i // 2

        @pl.when(far == 1)
        def _():
            new = own.at[:, pl.ds(5, 3)]
            pltpu.make_async_copy(new, new, far_sem.at[c]).wait()

        spec[i] = image_signal(c, far)

        @pl.when(far == 1)
        def _():
            ref, sec = spec[i - 2 + 2 * c], spec[i - 2 * c]
            sends[c] = looked(ref, sec, scale, tpu_roll).reshape(devices, GROUP, LANES)
            give(c, 0, devices // 4)

    loop(0, 4, image_of)
    for c in range(2):
        give(c, devices // 4, devices)
    gather[0, me] = sends[0, me]

    for c in range(2):
        whole = gather.at[c, pl.ds(0, devices - (1, 0)[c])]
        pltpu.make_async_copy(whole, whole, back_recv.at[c]).wait()

    half = LANES // 2
    joined = jnp.concatenate([gather[0], gather[1]], 1).reshape(2 * rows, LANES)
    for h in range(2 * rows // LANES):
        lanes = slice(h * LANES, (h + 1) * LANES)
        both = joined[lanes].T
        out_ref[0, 0, :, lanes] = both[:half]
        out_ref[0, 1, :, lanes] = both[half:]

    for c in range(2):
        sent = own.at[pl.ds(0, devices - 1), tiles[c]]
        pltpu.make_async_copy(sent, sent, send_sem.at[c]).wait()
        new = own.at[:, pl.ds(5, 3)]
        pltpu.make_async_copy(new, new, pass_sem.at[c]).wait()
        whole = gather.at[c, pl.ds(0, devices - (1, 0)[c])]
        pltpu.make_async_copy(whole, whole, back_send.at[c]).wait()


def shards(slc, band_start, band_stop):
    devices = lax.axis_size("line")
    chips = devices // CORES
    _, parts, columns, inner = slc.shape
    rows = devices * GROUP
    half = LANES // 2
    assert columns == devices * 2 * GROUP and inner == 2 * LANES + half
    constants = [jnp.asarray(c) for c in tables(devices, inner)]
    hbm = pl.BlockSpec(memory_space=pltpu.HBM)
    dma = pltpu.SemaphoreType.DMA
    count = pltpu.SemaphoreType.REGULAR
    f32 = jnp.float32
    result = pl.pallas_call(
        functools.partial(kernel, chips, EARLY * devices // 8, inner),
        out_shape=pltpu.VMEM((1, parts, inner // LOOKS, columns), f32),
        in_specs=[hbm] * (3 + len(constants)),
        out_specs=pl.BlockSpec(memory_space=pltpu.VMEM),
        scratch_shapes=[
            pltpu.VMEM((parts, inner, columns), f32),
            pltpu.VMEM((devices, 5, 2 * GROUP, LANES), f32),
            pltpu.VMEM((devices, 11, 2 * GROUP, LANES), f32),
            pltpu.VMEM((4, rows, 2 * inner), f32),
            pltpu.VMEM((2, devices, GROUP, LANES), f32),
            pltpu.VMEM((2, devices, GROUP, LANES), f32),
            pltpu.VMEM((2, 2 * rows, 2 * rows), jnp.bfloat16),
            pltpu.SMEM(band_start.shape, jnp.int32),
            pltpu.SMEM(band_stop.shape, jnp.int32),
            *(pltpu.VMEM(c.shape, c.dtype) for c in constants),
            dma,
            dma((8,)),
            count((chips,)),
            count((chips,)),
            count,
            dma((2,)),
            dma((2, chips)),
            dma((2,)),
            dma((2,)),
            dma((2,)),
            dma((2,)),
        ],
        compiler_params=pltpu.CompilerParams(collective_id=0, has_side_effects=True),
    )(jnp.swapaxes(slc, 2, 3), band_start, band_stop, *constants)
    return jnp.swapaxes(result, 2, 3)


def solution(mesh):
    return jax.shard_map(
        shards,
        mesh=mesh,
        in_specs=(P("date", None, "stack", "line"), P(), P()),
        out_specs=P("date", None, "stack", "line"),
        check_vma=False,
    )
```

```python
import functools
import math

import jax
import jax.numpy as jnp
import numpy as np
from jax import lax
from jax.experimental import pallas as pl
from jax.experimental.pallas import tpu as pltpu
from jax.sharding import PartitionSpec as P

LOOKS = 5
CORES = 2
GROUP = 4
EARLY = 4
LANES = 128
MESH = pl.DeviceIdType.MESH


def split_table(table):
    high = table.astype(jnp.bfloat16)
    low = (table - high.astype(np.float32)).astype(jnp.bfloat16)
    return np.stack([high, low])


@functools.lru_cache(maxsize=None)
def tables(outer, inner):
    whole = outer * inner
    bins = 2 * LANES
    tail = inner - bins
    eye = np.eye(GROUP)
    turn = 2 * np.pi / outer * (np.outer(np.arange(outer), np.arange(outer)) % outer)
    cos, sin = np.cos(turn), np.sin(turn)
    blocks = np.array([[cos, sin], [-sin, cos]])
    first = np.einsum("pqkd,x->pkdqx", blocks, np.ones(GROUP)).reshape(2 * outer, -1)
    last = np.einsum("qdk,cx->dcqxk", np.array([cos, sin]), eye).reshape(outer * GROUP, -1)
    line, bin_ = np.arange(inner), np.arange(bins)
    turn = 2 * np.pi / inner * (np.outer(line, bin_) % inner)
    cos, sin = np.cos(turn), np.sin(turn)
    from_re = np.concatenate([cos, -sin], 1)
    from_im = np.concatenate([sin, cos], 1)
    ahead = np.concatenate([from_re[:bins], from_im[:bins], from_re[bins:], from_im[bins:]])
    looks = inner // LOOKS
    order = (np.arange(looks)[None] * LOOKS + np.arange(LOOKS)[:, None]).reshape(-1)
    cos_o, sin_o = cos[order].T, sin[order].T
    to_re = np.concatenate([cos_o, -sin_o], 0).reshape(2 * bins, LOOKS, 1, looks)
    to_im = np.concatenate([sin_o, cos_o], 0).reshape(2 * bins, LOOKS, 1, looks)
    back = np.concatenate([to_re, to_im], 2).reshape(2 * bins, 2 * inner)
    k1 = np.arange(outer)
    lanes = np.concatenate([line, line[bins:]])
    turn = 2 * np.pi / whole * np.outer(k1, lanes)
    ahead_turn = np.stack([np.cos(turn), -np.sin(turn)])
    turn = 2 * np.pi / whole * np.outer(k1, order)
    cos, sin = (f(turn).reshape(-1, LOOKS, 1, looks) for f in (np.cos, np.sin))
    back_turn = np.stack(
        [
            np.concatenate([cos, cos], 2).reshape(-1, 2 * inner),
            np.concatenate([-sin, sin], 2).reshape(-1, 2 * inner),
        ]
    )
    assert 2 * tail == LANES and 2 * looks == LANES
    as_f32 = lambda a: a.astype(np.float32)
    return (
        split_table(as_f32(first)),
        split_table(as_f32(ahead)),
        split_table(as_f32(back)),
        split_table(as_f32(last)),
        as_f32(ahead_turn),
        as_f32(back_turn),
    )


def parts_of(values):
    high = values.astype(jnp.bfloat16)
    return high, (values - high.astype(jnp.float32)).astype(jnp.bfloat16)


def dot(a, b):
    return jnp.dot(a, b, preferred_element_type=jnp.float32)


def left(table, values):
    high, low = parts_of(values)
    return dot(table[0], high) + dot(table[0], low) + dot(table[1], high)


def right(values, table):
    high, low = parts_of(values)
    return dot(high, table[0]) + dot(low, table[0]) + dot(high, table[1])


def half_turned(values, roll):
    pieces = [
        roll(values[:, i : i + LANES]) for i in range(0, values.shape[1], LANES)
    ]
    return jnp.concatenate(pieces, 1)


def lane_index(shape):
    return lax.broadcasted_iota(jnp.int32, shape, 1)


def low_half(shape):
    return lane_index(shape) % LANES < LANES // 2


def start_turn(ahead_turn, start, outer, inner):
    lanes = lane_index((1, 3 * LANES))
    line = jnp.where(lanes < inner, lanes, lanes - (LANES // 2))
    steps = (line * (start // outer)).astype(jnp.float32)
    steps = steps - inner * jnp.floor((steps + 0.5) * (1.0 / inner))
    angle = steps * (2.0 * math.pi / inner)
    cos, sin = jnp.cos(angle), -jnp.sin(angle)
    real, imag = ahead_turn[0], ahead_turn[1]
    return for_columns(real * cos - imag * sin), for_columns(real * sin + imag * cos)


def first_table(first, outer):
    column = lane_index((2 * outer, first.shape[2])) % GROUP
    pieces = []
    for piece in (first[0], first[1]):
        wide = piece.astype(jnp.float32)
        own = [jnp.where(column == c, wide, 0.0) for c in range(GROUP)]
        rows = [v[:outer] for v in own] + [v[outer:] for v in own]
        pieces.append(jnp.concatenate(rows, 0).astype(jnp.bfloat16))
    return pieces


def for_columns(table):
    return jnp.concatenate([table] * GROUP, 0)


def lines_of(first, tiles, turn, second, roll):
    block = jnp.concatenate(tiles, 1)
    mixed = left(first, block)
    rows = mixed.shape[0] // 2
    real, imag = mixed[:rows], mixed[rows:]
    turned_real = real * turn[0] - imag * turn[1]
    turned_imag = real * turn[1] + imag * turn[0]
    main = 2 * LANES
    tail_real, tail_imag = turned_real[:, main:], turned_imag[:, main:]
    low = low_half(tail_real.shape)
    tail = jnp.where(
        second,
        jnp.where(low, roll(tail_real), tail_imag),
        jnp.where(low, tail_real, roll(tail_imag)),
    )
    return jnp.concatenate([turned_real[:, :main], turned_imag[:, :main], tail], 1)


def keep_mask(start, stop, outer, rows):
    shape = (rows, 2 * LANES)
    k1 = lax.broadcasted_iota(jnp.int32, shape, 0) % outer
    k = k1 + outer * (lane_index(shape) + start // outer)
    return (k >= start) & (k < stop)


def back_lines(spectrum, mask, back, back_turn, roll):
    bins = mask.shape[1]
    kept = jnp.concatenate(
        [jnp.where(mask, spectrum[:, :bins], 0.0), jnp.where(mask, spectrum[:, bins:], 0.0)], 1
    )
    lines = right(kept, back)
    return lines * for_columns(back_turn[0]) + half_turned(lines, roll) * for_columns(back_turn[1])


def signal_of(lines, last, roll):
    turned = half_turned(lines, roll)
    turned = jnp.where(low_half(turned.shape), -turned, turned)
    return left(last, jnp.concatenate([lines, turned], 0))


def looked(ref, sec, scale, roll):
    same = cross = None
    for i in range(LOOKS):
        a, b = (v[:, i * LANES : (i + 1) * LANES] for v in (ref, sec))
        one, two = a * b, a * roll(b)
        same = one if same is None else same + one
        cross = two if cross is None else cross + two
    low = low_half(same.shape)
    return jnp.where(low, same + roll(same), cross - roll(cross)) * scale


def tpu_roll(values):
    return pltpu.roll(values, LANES // 2, 1)


def ring_order(size):
    order = [size // 2]
    for step in range(size // 2 - 1, 0, -1):
        order += [step, size - step]
    return order


def sublanes_turned(values):
    return pltpu.roll(values, GROUP, 1)


def pack(image, packed, inner):
    columns = image.shape[2]
    for h in range(columns // LANES):
        lanes = slice(h * LANES, (h + 1) * LANES)
        count = LANES // (2 * GROUP)
        to = slice(h * count, (h + 1) * count)
        shape = (count, 2 * GROUP, LANES)
        upper = lax.broadcasted_iota(jnp.int32, shape, 1) < GROUP
        for k in range(2):
            lines = slice(k * LANES, (k + 1) * LANES)
            real, imag = (image[i, lines, lanes].T.reshape(shape) for i in range(2))
            packed[to, k] = jnp.where(upper, real, sublanes_turned(imag))
            packed[to, 3 + k] = jnp.where(upper, sublanes_turned(real), imag)
        tail = jnp.concatenate([image[i, 2 * LANES : inner, lanes] for i in range(2)], 0)
        tail = tail.T
        other = pltpu.roll(tail, LANES // 2, 1).reshape(shape)
        tail = tail.reshape(shape)
        low = lax.broadcasted_iota(jnp.int32, shape, 2) < LANES // 2
        packed[to, 2] = jnp.where(upper == low, tail, sublanes_turned(other))


def kernel(
    chips, early, inner,
    x_ref, start_hbm, stop_hbm,
    first_hbm, ahead_hbm, back_hbm, last_hbm, ahead_turn_hbm, back_turn_hbm,
    out_ref,
    image, packed, own, spec, sends, gather, mixing,
    start_ref, stop_ref, first, ahead, back, last, ahead_turn, back_turn,
    load_sem, table_sem, ready, known, prior, send_sem, own_sem, pass_sem, far_sem, back_send, back_recv,
):
    devices = chips * CORES
    me = lax.axis_index("line")
    chip = me // CORES
    partner = chip * CORES + (CORES - 1 - me % CORES)
    date = lax.axis_index("date")
    dates = lax.axis_size("date")
    before = lax.rem(date + dates - 1, dates)
    after = lax.rem(date + 1, dates)
    load = pltpu.make_async_copy(x_ref.at[0], image, load_sem)
    load.start()

    hubs = early - 1
    hub = (me >= 1) & (me < early)
    barrier = pltpu.get_barrier_semaphore()

    def signal(sem, line):
        pl.semaphore_signal(sem, 1, device_id={"line": line}, device_id_type=MESH)

    def loop(low, high, body):
        def step(i, _):
            body(i)
            return 0

        lax.fori_loop(low, high, step, 0)

    def others(low, high, body):
        loop(low, high, lambda i: pl.when(i != me)(lambda: body(i)))

    @pl.when(hub)
    def _():
        others(0, devices, lambda t: signal(barrier, t))

    for row in (before, after):
        pl.semaphore_signal(barrier, 1, device_id={"date": row}, device_id_type=MESH)

    moves = [
        pltpu.make_async_copy(source, to, table_sem.at[i])
        for i, (source, to) in enumerate(
            (
                (first_hbm, first), (start_hbm, start_ref), (stop_hbm, stop_ref),
                (ahead_turn_hbm, ahead_turn), (ahead_hbm, ahead), (back_hbm, back),
                (back_turn_hbm, back_turn), (last_hbm, last),
            )
        )
    ]

    @pl.when(jnp.logical_not(hub))
    def _():
        pl.semaphore_wait(barrier, hubs + 2)
        loop(1, early, lambda t: signal(ready.at[chip], t))

    load.wait()
    for move in moves:
        move.start()
    pack(image, packed, inner)

    @pl.when(hub)
    def _():
        pl.semaphore_wait(barrier, hubs + 1)

    message = pl.ds(0, 5)
    order = ring_order(chips)

    def send(t):
        pltpu.make_async_remote_copy(
            packed.at[t], own.at[me, message], send_sem, own_sem.at[chip],
            device_id={"line": t}, device_id_type=MESH,
        ).start()

    def ring(body):
        for o in order:
            t = lax.rem(chip + o, chips) * CORES
            for core in range(CORES):
                body(t + core)
        body(partner)

    ring(lambda t: pl.when((t >= 1) & (t < early))(lambda: send(t)))

    def send_chip(k):
        for core in range(CORES):
            send(k * CORES + core)

    first_chip = early // CORES

    @pl.when(hub)
    def _():
        teller = me == 1

        def meet(k):
            pl.semaphore_wait(ready.at[k], CORES)

            @pl.when(teller)
            def _():
                for core in range(CORES):
                    signal(prior, k * CORES + core)
                loop(early, k * CORES, lambda t: signal(known.at[k], t))
                pl.when(k == chips - 1)(lambda: signal(known.at[k], 0))

            send_chip(k)

        loop(first_chip, chips - 1, meet)
        pl.semaphore_wait(ready.at[0], 1)

        @pl.when(teller)
        def _():
            signal(prior, 0)
            loop(early, devices - CORES, lambda t: signal(known.at[0], t))

        send(0)
        meet(chips - 1)

    @pl.when(jnp.logical_not(hub))
    def _():
        zero = me == 0
        end = chip == chips - 1
        pl.semaphore_wait(prior, 1)
        pl.when(jnp.logical_not(zero))(lambda: send(partner))
        pl.when(end)(lambda: send(0))
        loop(first_chip, jnp.where(zero, chips - 1, chip), send_chip)

        def meet(k):
            pl.semaphore_wait(known.at[k], 1)
            send_chip(k)

        loop(jnp.where(zero, chips, chip + 1), chips - 1, meet)

        @pl.when(jnp.logical_not(zero | end))
        def _():
            pl.semaphore_wait(known.at[0], 1)
            send(0)

        pl.when(jnp.logical_not(end))(lambda: meet(chips - 1))

    own[me, 0:5] = packed[me]
    for move in moves:
        move.wait()
    for i, piece in enumerate(first_table(first, devices)):
        mixing[i] = piece

    passed = (pl.ds(0, 3), pl.ds(2, 3))
    passed_to = (pl.ds(5, 3), pl.ds(8, 3))
    rows_to = (before, after)

    def pass_on(s, c):
        lines = pl.ds(s * CORES, CORES)
        pltpu.make_async_remote_copy(
            own.at[lines, passed[c]], own.at[lines, passed_to[c]], pass_sem.at[c], far_sem.at[c],
            device_id={"date": rows_to[c]}, device_id_type=MESH,
        ).start()

    def take(s, count):
        new = own.at[pl.ds(0, count), message]
        pltpu.make_async_copy(new, new, own_sem.at[s]).wait()
        for c in range(2):
            pass_on(s, c)

    rows = devices * GROUP
    scale = 1.0 / (LOOKS * float(devices * inner) ** 2)

    def tile(k):
        return own[:, k].reshape(2 * rows, LANES)

    def image_signal(c, far):
        pair = jnp.where(c == 0, date, before)
        start, stop = start_ref[pair], stop_ref[pair]
        turn = start_turn(ahead_turn, start, devices, inner)
        main = 3 * c + far * (5 + c)
        tail = 2 + far * (5 + c)
        block = [tile(main), tile(main + 1), tile(tail)]
        lines = lines_of(mixing, block, turn, c == 1, tpu_roll)
        mask = keep_mask(start, stop, devices, rows)
        kept = back_lines(right(lines, ahead), mask, back, back_turn, tpu_roll)
        return signal_of(kept, last, tpu_roll)

    def give(c, low, high):
        row = jnp.where(c == 0, date, before)

        def one(t):
            pltpu.make_async_remote_copy(
                sends.at[c, t], gather.at[c, me], back_send.at[c], back_recv.at[c],
                device_id={"line": t, "date": row}, device_id_type=MESH,
            ).start()

        loop(low, high, lambda t: pl.when((c == 1) | (t != me))(lambda: one(t)))

    take(chip, 1)
    loop(1, chips - 1, lambda s: pl.when(s != chip)(lambda: take(s, CORES)))
    pl.when(chip != 0)(lambda: take(0, CORES))
    pl.when(chip != chips - 1)(lambda: take(chips - 1, CORES))

    def image_of(i):
        c, far = lax.rem(i, 2), i // 2

        @pl.when(far == 1)
        def _():
            new = own.at[:, pl.ds(5, 3)]
            pltpu.make_async_copy(new, new, far_sem.at[c]).wait()

        spec[i] = image_signal(c, far)

        @pl.when(far == 1)
        def _():
            ref, sec = spec[i - 2 + 2 * c], spec[i - 2 * c]
            sends[c] = looked(ref, sec, scale, tpu_roll).reshape(devices, GROUP, LANES)
            give(c, 0, devices // 4)

    loop(0, 4, image_of)
    for c in range(2):
        give(c, devices // 4, devices)
    gather[0, me] = sends[0, me]

    for c in range(2):
        whole = gather.at[c, pl.ds(0, devices - (1, 0)[c])]
        pltpu.make_async_copy(whole, whole, back_recv.at[c]).wait()

    half = LANES // 2
    joined = jnp.concatenate([gather[0], gather[1]], 1).reshape(2 * rows, LANES)
    for h in range(2 * rows // LANES):
        lanes = slice(h * LANES, (h + 1) * LANES)
        both = joined[lanes].T
        out_ref[0, 0, :, lanes] = both[:half]
        out_ref[0, 1, :, lanes] = both[half:]

    sent = own.at[pl.ds(0, devices - 1), message]
    pltpu.make_async_copy(sent, sent, send_sem).wait()
    for c in range(2):
        new = own.at[:, pl.ds(5, 3)]
        pltpu.make_async_copy(new, new, pass_sem.at[c]).wait()
        whole = gather.at[c, pl.ds(0, devices - (1, 0)[c])]
        pltpu.make_async_copy(whole, whole, back_send.at[c]).wait()


def shards(slc, band_start, band_stop):
    devices = lax.axis_size("line")
    chips = devices // CORES
    _, parts, columns, inner = slc.shape
    rows = devices * GROUP
    half = LANES // 2
    assert columns == devices * 2 * GROUP and inner == 2 * LANES + half
    constants = [jnp.asarray(c) for c in tables(devices, inner)]
    hbm = pl.BlockSpec(memory_space=pltpu.HBM)
    dma = pltpu.SemaphoreType.DMA
    count = pltpu.SemaphoreType.REGULAR
    f32 = jnp.float32
    result = pl.pallas_call(
        functools.partial(kernel, chips, EARLY * devices // 8, inner),
        out_shape=pltpu.VMEM((1, parts, inner // LOOKS, columns), f32),
        in_specs=[hbm] * (3 + len(constants)),
        out_specs=pl.BlockSpec(memory_space=pltpu.VMEM),
        scratch_shapes=[
            pltpu.VMEM((parts, inner, columns), f32),
            pltpu.VMEM((devices, 5, 2 * GROUP, LANES), f32),
            pltpu.VMEM((devices, 11, 2 * GROUP, LANES), f32),
            pltpu.VMEM((4, rows, 2 * inner), f32),
            pltpu.VMEM((2, devices, GROUP, LANES), f32),
            pltpu.VMEM((2, devices, GROUP, LANES), f32),
            pltpu.VMEM((2, 2 * rows, 2 * rows), jnp.bfloat16),
            pltpu.SMEM(band_start.shape, jnp.int32),
            pltpu.SMEM(band_stop.shape, jnp.int32),
            *(pltpu.VMEM(c.shape, c.dtype) for c in constants),
            dma,
            dma((8,)),
            count((chips,)),
            count((chips,)),
            count,
            dma,
            dma((chips,)),
            dma((2,)),
            dma((2,)),
            dma((2,)),
            dma((2,)),
        ],
        compiler_params=pltpu.CompilerParams(collective_id=0, has_side_effects=True),
    )(jnp.swapaxes(slc, 2, 3), band_start, band_stop, *constants)
    return jnp.swapaxes(result, 2, 3)


def solution(mesh):
    return jax.shard_map(
        shards,
        mesh=mesh,
        in_specs=(P("date", None, "stack", "line"), P(), P()),
        out_specs=P("date", None, "stack", "line"),
        check_vma=False,
    )
```
